32 devices in a mesh: fsdp: 8 (over z, y), sp: 4 (over x, core).
Axes of the slice: x: 2, y: 2, z: 4, core: 2. Of those that a mesh axis runs over, the one named last changes fastest.
Arguments:
- tokens: bfloat16 [8, 512, 1536], P('fsdp', 'sp'), may hold values from -6 to 6
- modulation: float32 [8, 1, 6, 1536], P('fsdp'), may hold values from -4 to 4
- w_qkv: bfloat16 [1, 1536, 3, 1536], P(None, 'fsdp', None, 'sp'), may hold values from -0.15625 to 0.15625
- w_out: bfloat16 [1, 1536, 1536], P(None, 'sp', 'fsdp'), may hold values from -0.15625 to 0.15625
- w_in: bfloat16 [1, 1536, 6144], P(None, 'fsdp', 'sp'), may hold values from -0.15625 to 0.15625
- w_back: bfloat16 [1, 6144, 1536], P(None, 'sp', 'fsdp'), may hold values from -0.078125 to 0.078125
- out_grad: bfloat16 [8, 512, 1536], P('fsdp', 'sp'), may hold values from -6 to 6
Outputs:
- final_out: bfloat16 [8, 512, 1536], P('fsdp', 'sp')
- input_grad: float32 [8, 512, 1536], P('fsdp', 'sp')
- grad_qkv: float32 [1, 1536, 3, 1536], P(None, 'fsdp', None, 'sp')
- grad_out: float32 [1, 1536, 1536], P(None, 'sp', 'fsdp')
- grad_in: float32 [1, 1536, 6144], P(None, 'fsdp', 'sp')
- grad_back: float32 [1, 6144, 1536], P(None, 'sp', 'fsdp')
The draws below stay inside these ranges and needn't reach their ends.
All inputs are finite; a program needn't handle non-finite values.
Results may differ from the reference program's by a relative error of at most 0.03.
Values may be sent and summed in bfloat16 or wider, within the bound.
A program may use at most 128 MiB of HBM per device.

```python
import math
import jax
import jax.numpy as jnp
from jax import lax

D = 1536
HEAD_DIM = 128
FF = 6144
LAYERS = 1
SEQ = 512
BATCH = 8
N_FSDP = 8


def block_scale(rng, dims, shards, smallest, top_value):
    def one(axis_at, parts):
        heights = jax.random.uniform(jax.random.fold_in(jax.random.fold_in(rng, 6), axis_at), (parts,), jnp.float32, smallest / len(shards), top_value / len(shards))
        return jnp.repeat(jnp.exp(heights), dims[axis_at] // parts).reshape((-1,) + (1,) * (len(dims) - axis_at - 1))

    gain = one(*shards[0])
    for cut in shards[1:]:
        gain = gain * one(*cut)
    return gain


def bell_draw(stream_key, shape, spread, limit, cuts=(), dtype=jnp.bfloat16):
    drawn = spread * jax.random.normal(stream_key, shape, jnp.float32)
    if cuts:
        drawn = drawn * block_scale(stream_key, shape, cuts, -0.22, 0.18)
    return jnp.clip(drawn, -limit, limit).astype(dtype)


def setup_inputs(seed: int = 0) -> dict:
    keys = jax.random.split(jax.random.key(seed), 8)
    tokens = bell_draw(keys[0], (BATCH, SEQ, D), 1.0, 6.0, ((0, 8), (1, 4)))
    modulation = bell_draw(keys[1], (BATCH, LAYERS, 6, D), 1.0, 4.0, ((0, 8),), jnp.float32)
    w_qkv = bell_draw(keys[2], (LAYERS, D, 3, D), D ** -0.5, 0.15625, ((1, 8), (3, 4)))
    w_out = bell_draw(keys[3], (LAYERS, D, D), D ** -0.5, 0.15625, ((1, 4), (2, 8)))
    w_in = bell_draw(keys[4], (LAYERS, D, FF), D ** -0.5, 0.15625, ((1, 8), (2, 4)))
    w_back = bell_draw(keys[5], (LAYERS, FF, D), FF ** -0.5, 0.078125, ((1, 4), (2, 8)))
    out_grad = bell_draw(keys[6], (BATCH, SEQ, D), 1.0, 6.0, ((0, 8), (1, 4)))
    return dict(tokens=tokens, modulation=modulation, w_qkv=w_qkv, w_out=w_out, w_in=w_in, w_back=w_back, out_grad=out_grad)


ln_eps = 1e-06
temper = 2.5
block_limit = 512

def normalize(stream):
    mean_part = lax.optimization_barrier(jnp.mean(stream, axis=-1, keepdims=True))
    centred = stream - mean_part
    rstd = lax.rsqrt(lax.optimization_barrier(jnp.mean(centred * centred, axis=-1, keepdims=True)) + ln_eps)
    return (centred * rstd, rstd)

def norm_back(normed, rstd, incoming):
    first = lax.optimization_barrier(jnp.mean(incoming, axis=-1, keepdims=True))
    second = lax.optimization_barrier(jnp.mean(incoming * normed, axis=-1, keepdims=True))
    return rstd * (incoming - first - normed * second)

def gelu_tanh(hidden):
    return jax.nn.gelu(hidden, approximate=True)

def project(left, weight):
    flat_rows = left.reshape(-1, left.shape[-1])
    result = jnp.dot(flat_rows, weight, preferred_element_type=jnp.float32)
    return result.reshape(left.shape[:-1] + (weight.shape[1],))

def project_back(left, weight):
    flat_rows = left.reshape(-1, left.shape[-1])
    result = lax.dot_general(flat_rows, weight, (((1,), (1,)), ((), ())), preferred_element_type=jnp.float32)
    return result.reshape(left.shape[:-1] + (weight.shape[0],))

def group_grad(left, right, grad_scale):
    width_left = left.shape[-1]
    width_right = right.shape[-1]
    left_groups = left.reshape(N_FSDP, -1, width_left)
    right_groups = right.reshape(N_FSDP, -1, width_right)

    def add_group(total, pair):
        left_part, right_part = pair
        term = lax.dot_general(left_part, right_part, (((0,), (0,)), ((), ())), preferred_element_type=jnp.float32) * grad_scale
        rounded = lax.optimization_barrier(term.astype(jnp.bfloat16))
        return (total + rounded.astype(jnp.float32), None)
    total, unused = lax.scan(add_group, jnp.zeros((width_left, width_right), jnp.float32), (left_groups, right_groups))
    return total

def split_heads(packed, head_count):
    return packed.reshape(packed.shape[:-1] + (head_count, packed.shape[-1] // head_count))

def heads_major(tensor):
    videos, seq_len, head_count, head_width = tensor.shape
    return tensor.transpose(0, 2, 1, 3).reshape(videos * head_count, seq_len, head_width)

def heads_minor(tensor, videos):
    merged, seq_len, head_width = tensor.shape
    return tensor.reshape(videos, merged // videos, seq_len, head_width).transpose(0, 2, 1, 3)

def attend_head(triple):
    queries, key_rows, values = triple
    seq_len, head_width = queries.shape
    block_size = min(block_limit, seq_len)
    score_factor = temper / math.sqrt(head_width)
    values_wide = values.astype(jnp.float32)

    def one_block(query_rows):
        scores = jnp.dot(query_rows, key_rows.T, preferred_element_type=jnp.float32) * score_factor
        softmaxed = jax.nn.softmax(scores, axis=-1)
        return jnp.dot(softmaxed, values_wide, precision=lax.Precision.HIGHEST).astype(jnp.bfloat16)
    attended = lax.map(one_block, queries.reshape(seq_len // block_size, block_size, head_width))
    return attended.reshape(seq_len, head_width)

def attend_back(quadruple):
    queries, key_rows, values, upstream = quadruple
    seq_len, head_width = queries.shape
    block_size = min(block_limit, seq_len)
    score_factor = temper / math.sqrt(head_width)
    keys_wide = key_rows.astype(jnp.float32)

    def one_block(running, block_pair):
        query_rows, grad_rows = block_pair
        scores = jnp.dot(query_rows, key_rows.T, preferred_element_type=jnp.float32) * score_factor
        softmaxed = jax.nn.softmax(scores, axis=-1)
        dprobs = jnp.dot(grad_rows, values.T, preferred_element_type=jnp.float32)
        dscores = softmaxed * (dprobs - lax.optimization_barrier(jnp.sum(softmaxed * dprobs, axis=-1, keepdims=True))) * score_factor
        dquery = jnp.dot(dscores, keys_wide, precision=lax.Precision.HIGHEST)
        grad_keys = running[0] + jnp.dot(dscores.T, query_rows.astype(jnp.float32), precision=lax.Precision.HIGHEST)
        dvalues = running[1] + jnp.dot(softmaxed.T, grad_rows.astype(jnp.float32), precision=lax.Precision.HIGHEST)
        return ((grad_keys, dvalues), dquery)
    zero_rows = jnp.zeros((seq_len, head_width), jnp.float32)
    count = seq_len // block_size
    blocks = (queries.reshape(count, block_size, head_width), upstream.reshape(count, block_size, head_width))
    (grad_keys, dvalues), dquery = lax.scan(one_block, (zero_rows, zero_rows), blocks)
    return (dquery.reshape(seq_len, head_width).astype(jnp.bfloat16), grad_keys.astype(jnp.bfloat16), dvalues.astype(jnp.bfloat16))

def attend_all(queries, key_rows, values):
    attended = lax.map(attend_head, (heads_major(queries), heads_major(key_rows), heads_major(values)))
    return heads_minor(attended, queries.shape[0])

def attend_all_back(queries, key_rows, values, upstream):
    grad_heads = lax.map(attend_back, (heads_major(queries), heads_major(key_rows), heads_major(values), heads_major(upstream)))
    return tuple((heads_minor(grad_piece, queries.shape[0]) for grad_piece in grad_heads))

def reference(tokens, modulation, w_qkv, w_out, w_in, w_back, out_grad):
    videos, seq_len, model_width = tokens.shape
    layers = w_qkv.shape[0]
    head_count = model_width // HEAD_DIM
    grad_scale = 1.0 / math.sqrt(videos * seq_len)
    stream = tokens.astype(jnp.float32)
    stored = []
    for layer_index in range(layers):
        layer_mod = modulation[:, layer_index][:, :, None, :]
        joint = w_qkv[layer_index].reshape(model_width, 3 * model_width)
        normed_first, rstd_first = normalize(stream)
        input_first = (normed_first * (1.0 + layer_mod[:, 1]) + layer_mod[:, 0]).astype(jnp.bfloat16)
        packed = project(input_first, joint).astype(jnp.bfloat16)
        queries = split_heads(packed[..., :model_width], head_count)
        key_rows = split_heads(packed[..., model_width:2 * model_width], head_count)
        values = split_heads(packed[..., 2 * model_width:], head_count)
        attended = attend_all(queries, key_rows, values).reshape(videos, seq_len, model_width)
        middle = stream + layer_mod[:, 2] * project(attended, w_out[layer_index])
        normed_second, rstd_second = normalize(middle)
        input_second = (normed_second * (1.0 + layer_mod[:, 4]) + layer_mod[:, 3]).astype(jnp.bfloat16)
        hidden = project(input_second, w_in[layer_index])
        activated = gelu_tanh(hidden).astype(jnp.bfloat16)
        stream = middle + layer_mod[:, 5] * project(activated, w_back[layer_index])
        stored.append((normed_first, rstd_first, input_first, queries, key_rows, values, attended, normed_second, rstd_second, input_second, hidden, activated))
    final_out = stream.astype(jnp.bfloat16)
    stream_grad = out_grad.astype(jnp.float32)
    results = [None] * layers
    for layer_index in range(layers - 1, -1, -1):
        normed_first, rstd_first, input_first, queries, key_rows, values, attended, normed_second, rstd_second, input_second, hidden, activated = stored[layer_index]
        layer_mod = modulation[:, layer_index][:, :, None, :]
        joint = w_qkv[layer_index].reshape(model_width, 3 * model_width)
        down_grad = (layer_mod[:, 5] * stream_grad).astype(jnp.bfloat16)
        back_hidden = project_back(down_grad, w_back[layer_index])
        unused, pullback = jax.vjp(gelu_tanh, hidden)
        up_grad = pullback(back_hidden)[0].astype(jnp.bfloat16)
        back_second = project_back(up_grad, w_in[layer_index])
        stream_grad = stream_grad + norm_back(normed_second, rstd_second, back_second * (1.0 + layer_mod[:, 4]))
        attn_grad = (layer_mod[:, 2] * stream_grad).astype(jnp.bfloat16)
        mixed_grad = split_heads(project_back(attn_grad, w_out[layer_index]).astype(jnp.bfloat16), head_count)
        grad_query, grad_keys, grad_values = attend_all_back(queries, key_rows, values, mixed_grad)
        packed_grad = jnp.concatenate([grad_query.reshape(videos, seq_len, model_width), grad_keys.reshape(videos, seq_len, model_width), grad_values.reshape(videos, seq_len, model_width)], axis=-1)
        back_first = project_back(packed_grad, joint)
        stream_grad = stream_grad + norm_back(normed_first, rstd_first, back_first * (1.0 + layer_mod[:, 1]))
        results[layer_index] = (group_grad(input_first, packed_grad, grad_scale).reshape(model_width, 3, model_width), group_grad(attended, attn_grad, grad_scale), group_grad(input_second, up_grad, grad_scale), group_grad(activated, down_grad, grad_scale))
    grad_qkv = jnp.stack([results[index][0] for index in range(layers)])
    grad_out = jnp.stack([results[index][1] for index in range(layers)])
    grad_in = jnp.stack([results[index][2] for index in range(layers)])
    grad_back = jnp.stack([results[index][3] for index in range(layers)])
    return (final_out, stream_grad, grad_qkv, grad_out, grad_in, grad_back)
```

```python
import functools
import math

import jax
import jax.numpy as jnp
from jax import lax
from jax.experimental import pallas as pl
from jax.experimental.pallas import tpu as pltpu
from jax.sharding import PartitionSpec as P

HEAD_DIM = 128
LN_EPS = 1e-06
TEMPER = 2.5
F32 = jnp.float32
BF16 = jnp.bfloat16


def ring_order(n):
    return list(range(0, n, 2)) + list(range(1, n, 2))[::-1]


def ring_tables(n):
    order = ring_order(n)
    right = [(order[p], order[(p + 1) % n]) for p in range(n)]
    left = [(order[p], order[(p - 1) % n]) for p in range(n)]
    place = [0] * n
    for p, device in enumerate(order):
        place[device] = p
    return jnp.array(order, jnp.int32), jnp.array(place, jnp.int32), right, left


def ring_at(distance):
    n = lax.axis_size("fsdp")
    order, place, _, _ = ring_tables(n)
    return order[(place[lax.axis_index("fsdp")] + distance + n) % n]


def ring_gather(block, swap):
    n = lax.axis_size("fsdp")
    _, _, right, left = ring_tables(n)
    rows = block.shape[0]
    whole = jnp.zeros((n * rows, block.shape[1]), block.dtype)
    whole = lax.dynamic_update_slice_in_dim(whole, block, lax.axis_index("fsdp") * rows, 0)
    far = n // 2
    reach = (n - 1 - far, far) if swap else (far, n - 1 - far)
    going = [block, block]
    for step in range(1, far + 1):
        for way, (pairs, sign) in enumerate(((right, -1), (left, 1))):
            if step <= reach[way]:
                going[way] = lax.ppermute(going[way], "fsdp", pairs)
                whole = lax.dynamic_update_slice_in_dim(
                    whole, going[way], ring_at(sign * step) * rows, 0
                )
    return whole


def ring_scatter(whole, swap):
    n = lax.axis_size("fsdp")
    _, _, right, left = ring_tables(n)
    rows = whole.shape[0] // n
    far = n // 2
    reach = (n - 1 - far, far) if swap else (far, n - 1 - far)

    def piece(distance):
        return lax.dynamic_slice_in_dim(whole, ring_at(distance) * rows, rows, 0)

    arrived = [None, None]
    for step in range(far, 0, -1):
        for way, (pairs, sign) in enumerate(((right, 1), (left, -1))):
            if step <= reach[way]:
                part = piece(sign * step)
                if arrived[way] is not None:
                    part = (part.astype(F32) + arrived[way].astype(F32)).astype(BF16)
                arrived[way] = lax.ppermute(part, "fsdp", pairs)
    total = piece(0).astype(F32)
    for part in arrived:
        if part is not None:
            total = total + part.astype(F32)
    return total


def core_swap(array):
    n = lax.axis_size("sp")
    return lax.ppermute(array, "sp", [(i, i ^ 1) for i in range(n)])


def chip_shift(array, step):
    n = lax.axis_size("sp")
    return lax.ppermute(array, "sp", [(i, (i + 2 * step) % n) for i in range(n)])


def seq_gather(block):
    n = lax.axis_size("sp")
    chips = n // 2
    index = lax.axis_index("sp")
    chip, core = index // 2, index % 2
    videos, own, width = block.shape
    pairs = []
    for step in range(chips):
        same = block if step == 0 else chip_shift(block, step)
        other = core_swap(same)
        low = jnp.where(core == 0, same, other)
        high = jnp.where(core == 0, other, same)
        pairs.append(jnp.stack([low, high], axis=1))
    if chips == 2:
        first = jnp.where(chip == 0, pairs[0], pairs[1])
        second = jnp.where(chip == 0, pairs[1], pairs[0])
        stacked = jnp.stack([first, second], axis=1)
    else:
        stacked = jnp.stack([pairs[0]] * chips, axis=1)
        for step in range(1, chips):
            stacked = lax.dynamic_update_slice_in_dim(
                stacked, pairs[step][:, None], (chip - step + chips) % chips, 1
            )
        stacked = lax.dynamic_update_slice_in_dim(stacked, pairs[0][:, None], chip, 1)
    return stacked.reshape(videos, n * own, width)


def seq_scatter(whole):
    n = lax.axis_size("sp")
    chips = n // 2
    index = lax.axis_index("sp")
    chip, core = index // 2, index % 2
    videos, positions, width = whole.shape
    split = whole.reshape(videos, chips, 2, positions // n, width)
    mine = lax.dynamic_index_in_dim(split, core, 2, keepdims=False)
    theirs = lax.dynamic_index_in_dim(split, 1 - core, 2, keepdims=False)
    both = (mine.astype(F32) + core_swap(theirs).astype(F32)).astype(BF16)
    total = lax.dynamic_index_in_dim(both, chip, 1, keepdims=False).astype(F32)
    for step in range(1, chips):
        part = lax.dynamic_index_in_dim(both, (chip + step) % chips, 1, keepdims=False)
        total = total + chip_shift(part, step).astype(F32)
    return total


def normalize(stream):
    centred = stream - jnp.mean(stream, axis=-1, keepdims=True)
    rstd = lax.rsqrt(jnp.mean(centred * centred, axis=-1, keepdims=True) + LN_EPS)
    return (centred * rstd, rstd)


def norm_back(normed, rstd, incoming):
    first = jnp.mean(incoming, axis=-1, keepdims=True)
    second = jnp.mean(incoming * normed, axis=-1, keepdims=True)
    return rstd * (incoming - first - normed * second)


def gelu_tanh(hidden):
    return jax.nn.gelu(hidden, approximate=True)


def contract(left, right, left_dim, right_dim):
    return lax.dot_general(
        left, right, (((left_dim,), (right_dim,)), ((), ())), preferred_element_type=F32
    )


def softmax_rows(queries, key_rows, factor):
    scores = contract(queries, key_rows, 1, 1) * factor
    scores = jnp.exp(scores - jnp.max(scores, axis=-1, keepdims=True))
    return scores * (1.0 / jnp.sum(scores, axis=-1, keepdims=True))


def attend_kernel(factor, q_ref, k_ref, v_ref, o_ref):
    probs = softmax_rows(q_ref[...], k_ref[...], factor)
    o_ref[...] = contract(probs.astype(BF16), v_ref[...], 1, 0).astype(BF16)


def attend_back_kernel(factor, heads, q_ref, k_ref, v_ref, do_ref, out_ref):
    head = pl.program_id(1)
    queries, key_rows, upstream = q_ref[...], k_ref[...], do_ref[...]
    probs = softmax_rows(queries, key_rows, factor)
    dprobs = contract(upstream, v_ref[...], 1, 1)
    dscores = probs * (dprobs - jnp.sum(probs * dprobs, axis=-1, keepdims=True)) * factor
    dscores = dscores.astype(BF16)
    parts = (
        contract(dscores, key_rows, 1, 0),
        contract(dscores, queries, 0, 0),
        contract(probs.astype(BF16), upstream, 0, 0),
    )
    for place, part in enumerate(parts):
        column = pl.multiple_of((place * heads + head) * HEAD_DIM, HEAD_DIM)
        out_ref[:, pl.ds(column, HEAD_DIM)] = part.astype(BF16)


def column_spec(seq, heads, place):
    return pl.BlockSpec((seq, HEAD_DIM), lambda video, head: (video, place * heads + head))


def attend(packed, videos, heads, factor):
    seq = packed.shape[0] // videos
    return pl.pallas_call(
        functools.partial(attend_kernel, factor),
        out_shape=jax.ShapeDtypeStruct((packed.shape[0], heads * HEAD_DIM), BF16),
        grid=(videos, heads),
        in_specs=[column_spec(seq, heads, place) for place in range(3)],
        out_specs=column_spec(seq, heads, 0),
        cost_estimate=pl.CostEstimate(
            flops=videos * heads * seq * seq * HEAD_DIM * 8,
            bytes_accessed=packed.size * 4,
            transcendentals=videos * heads * seq * seq,
        ),
    )(packed, packed, packed)


def attend_back(packed, upstream, videos, heads, factor):
    seq = packed.shape[0] // videos
    return pl.pallas_call(
        functools.partial(attend_back_kernel, factor, heads),
        out_shape=jax.ShapeDtypeStruct(packed.shape, BF16),
        grid=(videos, heads),
        in_specs=[column_spec(seq, heads, place) for place in (0, 1, 2, 0)],
        out_specs=pl.BlockSpec((seq, packed.shape[1]), lambda video, head: (video, 0)),
        cost_estimate=pl.CostEstimate(
            flops=videos * heads * seq * seq * HEAD_DIM * 20,
            bytes_accessed=packed.size * 4,
            transcendentals=videos * heads * seq * seq,
        ),
    )(packed, packed, packed, upstream)


def local(tokens, modulation, w_qkv, w_out, w_in, w_back, out_grad):
    videos, local_seq, width = tokens.shape
    layers = w_qkv.shape[0]
    own_width = w_qkv.shape[3]
    heads = own_width // HEAD_DIM
    factor = TEMPER / math.sqrt(HEAD_DIM)
    n_sp = lax.axis_size("sp")
    rows = videos * local_seq * n_sp
    grad_scale = 1.0 / math.sqrt(rows * lax.axis_size("fsdp"))

    def flat(array):
        return array.reshape(rows, array.shape[-1])

    def deep(array):
        return array.reshape(videos, local_seq * n_sp, array.shape[-1])

    def grad_term(left, right):
        return (contract(left, right, 0, 0) * grad_scale).astype(BF16)

    stream = tokens.astype(F32)
    stored = []
    for layer in range(layers):
        mod = modulation[:, layer][:, :, None, :]
        block_attn = jnp.concatenate(
            [w_qkv[layer].reshape(-1, 3 * own_width), w_out[layer].T], axis=1
        )
        whole_attn = ring_gather(block_attn, False)
        whole_in = ring_gather(w_in[layer], True)
        whole_back = ring_gather(w_back[layer].T, False)
        joint = whole_attn[:, : 3 * own_width]
        whole_out = whole_attn[:, 3 * own_width :]

        n1, r1 = normalize(stream)
        a1 = flat(seq_gather((n1 * (1.0 + mod[:, 1]) + mod[:, 0]).astype(BF16)))
        packed = contract(a1, joint, 1, 0).astype(BF16)
        attended = attend(packed, videos, heads, factor)
        attn_part = seq_scatter(deep(contract(attended, whole_out, 1, 1).astype(BF16)))
        middle = stream + mod[:, 2] * attn_part
        n2, r2 = normalize(middle)
        a2 = flat(seq_gather((n2 * (1.0 + mod[:, 4]) + mod[:, 3]).astype(BF16)))
        hidden = contract(a2, whole_in, 1, 0)
        active = gelu_tanh(hidden).astype(BF16)
        ffn_part = seq_scatter(deep(contract(active, whole_back, 1, 1).astype(BF16)))
        stream = middle + mod[:, 5] * ffn_part
        stored.append(
            (mod, joint, whole_out, whole_in, whole_back)
            + (n1, r1, a1, packed, attended, n2, r2, a2, hidden, active)
        )
    final_out = stream.astype(BF16)
    grad = out_grad.astype(F32)
    results = [None] * layers
    for layer in range(layers - 1, -1, -1):
        mod, joint, whole_out, whole_in, whole_back = stored[layer][:5]
        n1, r1, a1, packed, attended, n2, r2, a2, hidden, active = stored[layer][5:]
        dm = flat(seq_gather((mod[:, 5] * grad).astype(BF16)))
        sum_back = ring_scatter(grad_term(dm, active), False)
        dg = contract(dm, whole_back, 1, 0)
        _, pullback = jax.vjp(gelu_tanh, hidden)
        du = pullback(dg)[0].astype(BF16)
        back_second = seq_scatter(deep(contract(du, whole_in, 1, 1).astype(BF16)))
        sum_in = ring_scatter(grad_term(a2, du), True)
        grad = grad + norm_back(n2, r2, back_second * (1.0 + mod[:, 4]))
        da = flat(seq_gather((mod[:, 2] * grad).astype(BF16)))
        do = contract(da, whole_out, 1, 0).astype(BF16)
        dqkv = attend_back(packed, do, videos, heads, factor)
        back_first = seq_scatter(deep(contract(dqkv, joint, 1, 1).astype(BF16)))
        term_attn = jnp.concatenate([grad_term(a1, dqkv), grad_term(da, attended)], axis=1)
        sum_attn = ring_scatter(term_attn, False)
        grad = grad + norm_back(n1, r1, back_first * (1.0 + mod[:, 1]))
        results[layer] = (
            sum_attn[:, : 3 * own_width].reshape(-1, 3, own_width),
            sum_attn[:, 3 * own_width :].T,
            sum_in,
            sum_back.T,
        )
    grads = [jnp.stack([results[i][k] for i in range(layers)]) for k in range(4)]
    return (final_out, grad, *grads)


def solution(mesh):
    weights = (
        P(None, "fsdp", None, "sp"),
        P(None, "sp", "fsdp"),
        P(None, "fsdp", "sp"),
        P(None, "sp", "fsdp"),
    )
    rows = P("fsdp", "sp", None)
    return jax.shard_map(
        local,
        mesh=mesh,
        in_specs=(rows, P("fsdp", None, None, None), *weights, rows),
        out_specs=(rows, rows, *weights),
        check_vma=False,
    )
```

```python
import functools
import math

import jax
import jax.numpy as jnp
from jax import lax
from jax.experimental import pallas as pl
from jax.experimental.pallas import tpu as pltpu
from jax.sharding import PartitionSpec as P

HEAD_DIM = 128
LN_EPS = 1e-06
TEMPER = 2.5
F32 = jnp.float32
BF16 = jnp.bfloat16


def ring_order(n):
    return list(range(0, n, 2)) + list(range(1, n, 2))[::-1]


def ring_tables(n):
    order = ring_order(n)
    right = [(order[p], order[(p + 1) % n]) for p in range(n)]
    left = [(order[p], order[(p - 1) % n]) for p in range(n)]
    place = [0] * n
    for p, device in enumerate(order):
        place[device] = p
    return jnp.array(order, jnp.int32), jnp.array(place, jnp.int32), right, left


def ring_at(distance):
    n = lax.axis_size("fsdp")
    order, place, _, _ = ring_tables(n)
    return order[(place[lax.axis_index("fsdp")] + distance + n) % n]


def after(array, earlier):
    return array if earlier is None else lax.optimization_barrier((array, earlier))[0]


def ring_gather(block, swap, earlier=None):
    block = after(block, earlier)
    n = lax.axis_size("fsdp")
    _, _, right, left = ring_tables(n)
    rows = block.shape[0]
    whole = jnp.zeros((n * rows, block.shape[1]), block.dtype)
    whole = lax.dynamic_update_slice_in_dim(whole, block, lax.axis_index("fsdp") * rows, 0)
    far = n // 2
    reach = (n - 1 - far, far) if swap else (far, n - 1 - far)
    going = [block, block]
    for step in range(1, far + 1):
        for way, (pairs, sign) in enumerate(((right, -1), (left, 1))):
            if step <= reach[way]:
                going[way] = lax.ppermute(going[way], "fsdp", pairs)
                whole = lax.dynamic_update_slice_in_dim(
                    whole, going[way], ring_at(sign * step) * rows, 0
                )
        if step == max(1, far - 1):
            late = tuple(going)
    return whole, late


def ring_scatter(whole, swap):
    n = lax.axis_size("fsdp")
    _, _, right, left = ring_tables(n)
    rows = whole.shape[0] // n
    far = n // 2
    reach = (n - 1 - far, far) if swap else (far, n - 1 - far)

    def piece(distance):
        return lax.dynamic_slice_in_dim(whole, ring_at(distance) * rows, rows, 0)

    arrived = [None, None]
    for step in range(far, 0, -1):
        for way, (pairs, sign) in enumerate(((right, 1), (left, -1))):
            if step <= reach[way]:
                part = piece(sign * step)
                if arrived[way] is not None:
                    part = (part.astype(F32) + arrived[way].astype(F32)).astype(BF16)
                arrived[way] = lax.ppermute(part, "fsdp", pairs)
    total = piece(0).astype(F32)
    for part in arrived:
        if part is not None:
            total = total + part.astype(F32)
    return total


def core_swap(array):
    n = lax.axis_size("sp")
    return lax.ppermute(array, "sp", [(i, i ^ 1) for i in range(n)])


def chip_shift(array, step):
    n = lax.axis_size("sp")
    return lax.ppermute(array, "sp", [(i, (i + 2 * step) % n) for i in range(n)])


def seq_gather(block):
    n = lax.axis_size("sp")
    chips = n // 2
    index = lax.axis_index("sp")
    chip, core = index // 2, index % 2
    videos, own, width = block.shape
    pairs = []
    for step in range(chips):
        same = block if step == 0 else chip_shift(block, step)
        other = core_swap(same)
        low = jnp.where(core == 0, same, other)
        high = jnp.where(core == 0, other, same)
        pairs.append(jnp.stack([low, high], axis=1))
    if chips == 2:
        first = jnp.where(chip == 0, pairs[0], pairs[1])
        second = jnp.where(chip == 0, pairs[1], pairs[0])
        stacked = jnp.stack([first, second], axis=1)
    else:
        stacked = jnp.stack([pairs[0]] * chips, axis=1)
        for step in range(1, chips):
            stacked = lax.dynamic_update_slice_in_dim(
                stacked, pairs[step][:, None], (chip - step + chips) % chips, 1
            )
        stacked = lax.dynamic_update_slice_in_dim(stacked, pairs[0][:, None], chip, 1)
    return stacked.reshape(videos, n * own, width)


def seq_scatter(whole):
    n = lax.axis_size("sp")
    chips = n // 2
    index = lax.axis_index("sp")
    chip, core = index // 2, index % 2
    videos, positions, width = whole.shape
    split = whole.reshape(videos, chips, 2, positions // n, width)
    mine = lax.dynamic_index_in_dim(split, core, 2, keepdims=False)
    theirs = lax.dynamic_index_in_dim(split, 1 - core, 2, keepdims=False)
    both = (mine.astype(F32) + core_swap(theirs).astype(F32)).astype(BF16)
    total = lax.dynamic_index_in_dim(both, chip, 1, keepdims=False).astype(F32)
    for step in range(1, chips):
        part = lax.dynamic_index_in_dim(both, (chip + step) % chips, 1, keepdims=False)
        total = total + chip_shift(part, step).astype(F32)
    return total


def normalize(stream):
    centred = stream - jnp.mean(stream, axis=-1, keepdims=True)
    rstd = lax.rsqrt(jnp.mean(centred * centred, axis=-1, keepdims=True) + LN_EPS)
    return (centred * rstd, rstd)


def norm_back(normed, rstd, incoming):
    first = jnp.mean(incoming, axis=-1, keepdims=True)
    second = jnp.mean(incoming * normed, axis=-1, keepdims=True)
    return rstd * (incoming - first - normed * second)


def gelu_tanh(hidden):
    return jax.nn.gelu(hidden, approximate=True)


def contract(left, right, left_dim, right_dim):
    return lax.dot_general(
        left, right, (((left_dim,), (right_dim,)), ((), ())), preferred_element_type=F32
    )


def softmax_rows(queries, key_rows, factor):
    scores = contract(queries, key_rows, 1, 1) * factor
    scores = jnp.exp(scores - jnp.max(scores, axis=-1, keepdims=True))
    return scores * (1.0 / jnp.sum(scores, axis=-1, keepdims=True))


def attend_kernel(factor, q_ref, k_ref, v_ref, o_ref):
    probs = softmax_rows(q_ref[...], k_ref[...], factor)
    o_ref[...] = contract(probs.astype(BF16), v_ref[...], 1, 0).astype(BF16)


def attend_back_kernel(factor, heads, q_ref, k_ref, v_ref, do_ref, out_ref):
    head = pl.program_id(1)
    queries, key_rows, upstream = q_ref[...], k_ref[...], do_ref[...]
    probs = softmax_rows(queries, key_rows, factor)
    dprobs = contract(upstream, v_ref[...], 1, 1)
    dscores = probs * (dprobs - jnp.sum(probs * dprobs, axis=-1, keepdims=True)) * factor
    dscores = dscores.astype(BF16)
    parts = (
        contract(dscores, key_rows, 1, 0),
        contract(dscores, queries, 0, 0),
        contract(probs.astype(BF16), upstream, 0, 0),
    )
    for place, part in enumerate(parts):
        column = pl.multiple_of((place * heads + head) * HEAD_DIM, HEAD_DIM)
        out_ref[:, pl.ds(column, HEAD_DIM)] = part.astype(BF16)


def column_spec(seq, heads, place):
    return pl.BlockSpec((seq, HEAD_DIM), lambda video, head: (video, place * heads + head))


def attend(packed, videos, heads, factor):
    seq = packed.shape[0] // videos
    return pl.pallas_call(
        functools.partial(attend_kernel, factor),
        out_shape=jax.ShapeDtypeStruct((packed.shape[0], heads * HEAD_DIM), BF16),
        grid=(videos, heads),
        in_specs=[column_spec(seq, heads, place) for place in range(3)],
        out_specs=column_spec(seq, heads, 0),
        cost_estimate=pl.CostEstimate(
            flops=videos * heads * seq * seq * HEAD_DIM * 8,
            bytes_accessed=packed.size * 4,
            transcendentals=videos * heads * seq * seq,
        ),
    )(packed, packed, packed)


def attend_back(packed, upstream, videos, heads, factor):
    seq = packed.shape[0] // videos
    return pl.pallas_call(
        functools.partial(attend_back_kernel, factor, heads),
        out_shape=jax.ShapeDtypeStruct(packed.shape, BF16),
        grid=(videos, heads),
        in_specs=[column_spec(seq, heads, place) for place in (0, 1, 2, 0)],
        out_specs=pl.BlockSpec((seq, packed.shape[1]), lambda video, head: (video, 0)),
        cost_estimate=pl.CostEstimate(
            flops=videos * heads * seq * seq * HEAD_DIM * 20,
            bytes_accessed=packed.size * 4,
            transcendentals=videos * heads * seq * seq,
        ),
    )(packed, packed, packed, upstream)


def local(tokens, modulation, w_qkv, w_out, w_in, w_back, out_grad):
    videos, local_seq, width = tokens.shape
    layers = w_qkv.shape[0]
    own_width = w_qkv.shape[3]
    heads = own_width // HEAD_DIM
    factor = TEMPER / math.sqrt(HEAD_DIM)
    n_sp = lax.axis_size("sp")
    rows = videos * local_seq * n_sp
    grad_scale = 1.0 / math.sqrt(rows * lax.axis_size("fsdp"))

    def flat(array):
        return array.reshape(rows, array.shape[-1])

    def deep(array):
        return array.reshape(videos, local_seq * n_sp, array.shape[-1])

    def grad_term(left, right):
        return (contract(left, right, 0, 0) * grad_scale).astype(BF16)

    stream = tokens.astype(F32)
    stored = []
    for layer in range(layers):
        mod = modulation[:, layer][:, :, None, :]
        block_attn = jnp.concatenate(
            [w_qkv[layer].reshape(-1, 3 * own_width), w_out[layer].T], axis=1
        )
        whole_attn, late = ring_gather(block_attn, False)
        whole_in, late = ring_gather(w_in[layer], True, late)
        whole_back, late = ring_gather(w_back[layer].T, False, late)
        joint = whole_attn[:, : 3 * own_width]
        whole_out = whole_attn[:, 3 * own_width :]

        n1, r1 = normalize(stream)
        a1 = flat(seq_gather((n1 * (1.0 + mod[:, 1]) + mod[:, 0]).astype(BF16)))
        packed = contract(a1, joint, 1, 0).astype(BF16)
        attended = attend(packed, videos, heads, factor)
        attn_part = seq_scatter(deep(contract(attended, whole_out, 1, 1).astype(BF16)))
        middle = stream + mod[:, 2] * attn_part
        n2, r2 = normalize(middle)
        a2 = flat(seq_gather((n2 * (1.0 + mod[:, 4]) + mod[:, 3]).astype(BF16)))
        hidden = contract(a2, whole_in, 1, 0)
        active = gelu_tanh(hidden).astype(BF16)
        ffn_part = seq_scatter(deep(contract(active, whole_back, 1, 1).astype(BF16)))
        stream = middle + mod[:, 5] * ffn_part
        stored.append(
            (mod, joint, whole_out, whole_in, whole_back)
            + (n1, r1, a1, packed, attended, n2, r2, a2, hidden, active)
        )
    final_out = stream.astype(BF16)
    grad = out_grad.astype(F32)
    results = [None] * layers
    for layer in range(layers - 1, -1, -1):
        mod, joint, whole_out, whole_in, whole_back = stored[layer][:5]
        n1, r1, a1, packed, attended, n2, r2, a2, hidden, active = stored[layer][5:]
        dm = flat(seq_gather((mod[:, 5] * grad).astype(BF16)))
        sum_back = ring_scatter(grad_term(dm, active), False)
        dg = contract(dm, whole_back, 1, 0)
        _, pullback = jax.vjp(gelu_tanh, hidden)
        du = pullback(dg)[0].astype(BF16)
        back_second = seq_scatter(deep(contract(du, whole_in, 1, 1).astype(BF16)))
        sum_in = ring_scatter(grad_term(a2, du), True)
        grad = grad + norm_back(n2, r2, back_second * (1.0 + mod[:, 4]))
        da = flat(seq_gather((mod[:, 2] * grad).astype(BF16)))
        sum_out = ring_scatter(grad_term(da, attended), True)
        do = contract(da, whole_out, 1, 0).astype(BF16)
        dqkv = attend_back(packed, do, videos, heads, factor)
        back_first = seq_scatter(deep(contract(dqkv, joint, 1, 1).astype(BF16)))
        sum_qkv = ring_scatter(grad_term(a1, dqkv), False)
        grad = grad + norm_back(n1, r1, back_first * (1.0 + mod[:, 1]))
        results[layer] = (
            sum_qkv.reshape(-1, 3, own_width),
            sum_out.T,
            sum_in,
            sum_back.T,
        )
    grads = [jnp.stack([results[i][k] for i in range(layers)]) for k in range(4)]
    return (final_out, grad, *grads)


def solution(mesh):
    weights = (
        P(None, "fsdp", None, "sp"),
        P(None, "sp", "fsdp"),
        P(None, "fsdp", "sp"),
        P(None, "sp", "fsdp"),
    )
    rows = P("fsdp", "sp", None)
    return jax.shard_map(
        local,
        mesh=mesh,
        in_specs=(rows, P("fsdp", None, None, None), *weights, rows),
        out_specs=(rows, rows, *weights),
        check_vma=False,
    )
```
